32 devices in a mesh: gx: 8 (over y, x, core), gy: 4 (over z).
Axes of the slice: x: 2, y: 2, z: 4, core: 2. Of those that a mesh axis runs over, the one named last changes fastest.
Arguments:
- kernels: bfloat16 [4, 4, 512, 256, 128], P(None, None, 'gx', 'gy'), may hold values from -600 to 600
- event_weight: float32 [4], replicated, may hold values from 0.3 to 3
Outputs:
- smoothed: float32 [4, 512, 256, 128], P(None, 'gx', 'gy')
The draws below stay inside these ranges and needn't reach their ends.
All inputs are finite; a program needn't handle non-finite values.
Results may differ from the reference program's by a relative error of at most 0.0053.
Values may be sent and summed in bfloat16 or wider, within the bound.
A program may use at most 192 MiB of HBM per device.

```python
import math
import jax
import jax.numpy as jnp

BLOCK = 64
DEPTH = 128
PARAMS = 4
EVENTS = 4
RADIUS = 192
NX = 512
NY = 256


def block_scale(rng, extent, shards, smallest, high):
    gain, own = 1.0, jax.random.fold_in(rng, 6)
    for position, shards_of in shards:
        steps = jnp.exp(jax.random.uniform(jax.random.fold_in(own, position), (shards_of,), jnp.float32, smallest / len(shards), high / len(shards)))
        gain = gain * jnp.repeat(steps, extent[position] // shards_of).reshape([-1 if axis == position else 1 for axis in range(len(extent))])
    return gain


def gaussian(key, extent, deviation, bound, cuts=(), held_as=jnp.bfloat16):
    factor_of = block_scale(key, extent, cuts, -0.22, 0.18) if cuts else 1.0
    entries = jax.random.normal(key, extent, jnp.float32) * deviation * factor_of
    return jnp.minimum(jnp.maximum(entries, -bound), bound).astype(held_as)


def setup_inputs(seed: int = 0) -> dict:
    streams_of = jax.random.split(jax.random.key(seed), 3)
    return {
        "kernels": gaussian(streams_of[0], (EVENTS, PARAMS, NX, NY, DEPTH), 100.0, 600.0, ((2, 8), (3, 4))),
        "event_weight": jnp.clip(jnp.exp(jax.random.uniform(streams_of[1], (EVENTS,), jnp.float32, math.log(0.3), math.log(3.0))), 0.3, 3.0),
    }


def band_matrix(count, radius, sigma):
    rows = jnp.arange(count, dtype=jnp.int32)
    offsets = rows[None, :] - rows[:, None]
    values = offsets.astype(jnp.float32)
    weights = jnp.exp(-values * values / (2.0 * sigma * sigma))
    return jnp.where(jnp.abs(offsets) <= radius, weights, 0.0).astype(jnp.bfloat16)


def reference(kernels, event_weight):
    sigma = 2.0 * BLOCK
    summed = jnp.sum(event_weight[:, None, None, None, None] * kernels.astype(jnp.float32), axis=0).astype(jnp.bfloat16)
    mat_x = band_matrix(NX, RADIUS, sigma)
    norm_x = jnp.sum(mat_x.astype(jnp.float32), axis=1)
    flat = jnp.moveaxis(summed, 1, 0).reshape(NX, -1)
    along_x = jnp.dot(mat_x, flat, preferred_element_type=jnp.float32) / norm_x[:, None]
    along_x = along_x.astype(jnp.bfloat16).reshape(NX, PARAMS, NY, DEPTH)
    mat_y = band_matrix(NY, RADIUS, sigma)
    norm_y = jnp.sum(mat_y.astype(jnp.float32), axis=1)
    flat_y = jnp.moveaxis(along_x, 2, 0).reshape(NY, -1)
    result = jnp.dot(mat_y, flat_y, preferred_element_type=jnp.float32) / norm_y[:, None]
    result = result.reshape(NY, NX, PARAMS, DEPTH)
    result = jnp.moveaxis(result, 0, 2)
    return jnp.moveaxis(result, 1, 0)
```

```python
import functools
import jax
import jax.numpy as jnp
from jax import lax
from jax.experimental import pallas as pl
from jax.experimental.pallas import tpu as pltpu
from jax.sharding import PartitionSpec as P

REACH = 3
MESH = pl.DeviceIdType.MESH


def fill_band(mat, inv, radius, sigma):
    count = mat.shape[0]
    step = 64

    @pl.loop(0, count // step)
    def _(i):
        rows = lax.broadcasted_iota(jnp.int32, (step, count), 0) + i * step
        cols = lax.broadcasted_iota(jnp.int32, (step, count), 1)
        offsets = cols - rows
        values = offsets.astype(jnp.float32)
        weights = jnp.exp(-values * values / (2.0 * sigma * sigma))
        weights = jnp.where(jnp.abs(offsets) <= radius, weights, 0.0).astype(jnp.bfloat16)
        at = pl.ds(pl.multiple_of(i * step, step), step)
        mat[at, :] = weights
        norms = jnp.sum(weights.astype(jnp.float32), axis=1, keepdims=True)
        inv[at, :] = jnp.broadcast_to(1.0 / norms, (step, inv.shape[1]))


def smooth(mat, inv, src, dst, group):
    depth = src.shape[2]

    @pl.loop(0, src.shape[0] // group)
    def _(i):
        first = i * group
        rhs = jnp.concatenate([src[first + k] for k in range(group)], axis=1)
        out = jnp.dot(mat[...], rhs, preferred_element_type=jnp.float32)
        for k in range(group):
            piece = out[:, k * depth:(k + 1) * depth] * inv[...]
            dst[first + k] = piece.astype(dst.dtype)


def kernel(nx, ny, weight, data, out, inbuf, summed, ybuf, yout, yback, turned, xbuf, xout, xback,
           wide, mat_x, inv_x, mat_y, inv_y, in_sems, out_sems, own_sems, zs, zr, xs, xr):
    events, params, bx, by, depth = data.shape
    radius, sigma = REACH * bx, 2.0 * bx
    px, py = bx // ny, by // nx
    me_x, me_y = lax.axis_index("gx"), lax.axis_index("gy")
    half = params // 2
    z_first, x_first = list(range(half)), list(range(half, params))
    loads = [p for i in range(max(half, params - half)) for p in z_first[i:i + 1] + x_first[i:i + 1]]

    order = list(range(1, ny)) + [0]

    def load(i, d):
        rows = pl.ds(lax.rem(me_y + d, ny) * px, px)
        return [pltpu.make_async_copy(data.at[e, loads[i], rows], inbuf.at[i % 2, e, rows], in_sems.at[i, e, d])
                for e in range(events)]

    def start_load(i):
        for d in order:
            for c in load(i, d):
                c.start()

    for i in range(min(2, params)):
        start_load(i)

    barrier = pltpu.get_barrier_semaphore()
    for d in range(1, nx):
        pl.semaphore_signal(barrier, inc=1, device_id={"gx": lax.rem(me_x + d, nx)}, device_id_type=MESH)
    for d in range(1, ny):
        pl.semaphore_signal(barrier, inc=1, device_id={"gy": lax.rem(me_y + d, ny)}, device_id_type=MESH)
    pl.semaphore_wait(barrier, nx + ny - 2)

    sends = {}
    counter = [0]

    def exchange(name, axis, size, me, src_of, dst, send, recv, before=None):
        own = pltpu.make_async_copy(src_of(me), dst, own_sems.at[counter[0]])
        counter[0] += 1
        copies = []
        for d in range(1, size):
            peer = lax.rem(me + d, size)
            copies.append(pltpu.make_async_remote_copy(
                src_ref=src_of(peer), dst_ref=dst, send_sem=send.at[d - 1], recv_sem=recv.at[d - 1],
                device_id={axis: peer}, device_id_type=MESH))
        for d, c in list(enumerate(copies, 1)) + [(0, own)]:
            if before is not None:
                before(d)
            c.start()
        sends[name] = (copies, own)

    def arrived(name):
        copies, own = sends[name]
        for c in copies:
            c.wait_recv()
        own.wait()

    def sent(name):
        for c in sends[name][0]:
            c.wait_send()

    def z_out(p, before=None):
        exchange(("zf", p), "gy", ny, me_y, lambda j: summed.at[p, pl.ds(j * px, px)],
                 ybuf.at[p, :, pl.ds(pl.multiple_of(me_y * by, by), by)], zs.at[0, p], zr.at[0, p], before)

    def z_smooth(p):
        arrived(("zf", p))
        smooth(mat_y, inv_y, ybuf.at[p], yout.at[p], min(4, px))
        exchange(("zb", p), "gy", ny, me_y, lambda j: yout.at[p, :, pl.ds(pl.multiple_of(j * by, by), by)],
                 yback.at[p, pl.ds(me_y * px, px)], zs.at[1, p], zr.at[1, p])

    def x_out(p):
        exchange(("xf", p), "gx", nx, me_x, lambda j: turned.at[p, pl.ds(j * py, py)],
                 xbuf.at[p, :, pl.ds(pl.multiple_of(me_x * bx, bx), bx)], xs.at[0, p], xr.at[0, p])

    def x_smooth(p):
        arrived(("xf", p))
        smooth(mat_x, inv_x, xbuf.at[p], xout.at[p], min(4, py))
        exchange(("xb", p), "gx", nx, me_x, lambda j: xout.at[p, :, pl.ds(pl.multiple_of(j * bx, bx), bx)],
                 xback.at[p, pl.ds(me_x * py, py)], xs.at[1, p], xr.at[1, p])

    def widen(src):
        rows = src.shape[1]

        @pl.loop(0, src.shape[0])
        def _(i):
            wide[pl.ds(pl.multiple_of(i * rows, rows), rows), :] = src[i].astype(jnp.float32)

    def turn(dst, inner):
        @pl.loop(0, dst.shape[0])
        def _(j):
            dst[j] = wide[pl.ds(j, dst.shape[1], stride=inner), :].astype(dst.dtype)

    def add_up(i, into_wide, d):
        for c in load(i, d):
            c.wait()
        p, slot = loads[i], i % 2
        first = lax.rem(me_y + d, ny) * px
        scale = [weight[e] for e in range(events)]

        @pl.loop(0, px)
        def _(k):
            x = first + k
            total = scale[0] * inbuf[slot, 0, x].astype(jnp.float32)
            for e in range(1, events):
                total = total + scale[e] * inbuf[slot, e, x].astype(jnp.float32)
            if into_wide:
                wide[pl.ds(pl.multiple_of(x * by, by), by), :] = total
            else:
                summed[p, x] = total.astype(jnp.bfloat16)

    def x_to_z(p):
        arrived(("xb", p))
        widen(xback.at[p])
        turn(summed.at[p], bx)
        z_out(p)

    def z_to_x(p):
        arrived(("zb", p))
        widen(yback.at[p])
        turn(turned.at[p], by)
        x_out(p)

    for i, p in enumerate(loads):
        if p < half:
            z_out(p, functools.partial(add_up, i, False))
        else:
            for d in order:
                add_up(i, True, d)
            turn(turned.at[p], by)
            x_out(p)
        if i + 2 < params:
            start_load(i + 2)
    fill_band(mat_x, inv_x, radius, sigma)
    fill_band(mat_y, inv_y, radius, sigma)

    for i, b in enumerate(x_first):
        x_smooth(b)
        if i < half:
            z_smooth(z_first[i])
    for b in x_first:
        x_to_z(b)
    for i, b in enumerate(x_first):
        if i < half:
            z_to_x(z_first[i])
        if 0 < i <= half:
            x_smooth(z_first[i - 1])
        z_smooth(b)
    if half and half == len(x_first):
        x_smooth(z_first[-1])

    writes = []
    for i, b in enumerate(x_first):
        if i < half:
            a = z_first[i]
            arrived(("xb", a))
            widen(xback.at[a])
            sent(("zf", a))
            turn(summed.at[a], bx)
            writes.append(pltpu.make_async_copy(summed.at[a], out.at[a], out_sems.at[a, 0]))
            writes[-1].start()
        copies, own = sends[("zb", b)]
        for d in [0] + order[:-1]:
            if d:
                copies[d - 1].wait_recv()
            else:
                own.wait()
            rows = pl.ds(lax.rem(me_y + ny - d, ny) * px, px)
            writes.append(pltpu.make_async_copy(yback.at[b, rows], out.at[b, rows], out_sems.at[b, d]))
            writes[-1].start()
    for name in sends:
        if not (name[0] == "zf" and name[1] < half):
            sent(name)
    for c in writes:
        c.wait()


def body(nx, ny, kernels, event_weight):
    events, params, bx, by, depth = kernels.shape
    px, py = bx // ny, by // nx
    half = jnp.bfloat16
    block = (params, bx, by, depth)
    flipped = (params, by, bx, depth)
    y_lines = (params, px, by * ny, depth)
    x_lines = (params, py, bx * nx, depth)
    dma = pltpu.SemaphoreType.DMA
    smoothed = pl.pallas_call(
        functools.partial(kernel, nx, ny),
        out_shape=pltpu.VMEM(block, half),
        in_specs=[pl.BlockSpec(memory_space=pltpu.SMEM), pl.BlockSpec(memory_space=pl.ANY)],
        out_specs=pl.BlockSpec(memory_space=pltpu.VMEM),
        scratch_shapes=[
            pltpu.VMEM((2, events, bx, by, depth), half),
            pltpu.VMEM(block, half),
            pltpu.VMEM(y_lines, half),
            pltpu.VMEM(y_lines, half),
            pltpu.VMEM(block, half),
            pltpu.VMEM(flipped, half),
            pltpu.VMEM(x_lines, half),
            pltpu.VMEM(x_lines, half),
            pltpu.VMEM(flipped, half),
            pltpu.VMEM((bx * by, depth), jnp.float32),
            pltpu.VMEM((bx * nx, bx * nx), half),
            pltpu.VMEM((bx * nx, depth), jnp.float32),
            pltpu.VMEM((by * ny, by * ny), half),
            pltpu.VMEM((by * ny, depth), jnp.float32),
            dma((params, events, ny)),
            dma((params, ny)),
            dma((4 * params,)),
            dma((2, params, ny - 1)),
            dma((2, params, ny - 1)),
            dma((2, params, nx - 1)),
            dma((2, params, nx - 1)),
        ],
        compiler_params=pltpu.CompilerParams(collective_id=0, has_side_effects=True, vmem_limit_bytes=50 * 2**20),
    )(event_weight, kernels)
    return smoothed.astype(jnp.float32)


def solution(mesh):
    return jax.shard_map(
        functools.partial(body, mesh.shape["gx"], mesh.shape["gy"]),
        mesh=mesh,
        in_specs=(P(None, None, "gx", "gy", None), P()),
        out_specs=P(None, "gx", "gy", None),
        check_vma=False,
    )
```
